8 devices in a mesh: dp: 1 (over z), tp: 8 (over x, y, core).
Axes of the slice: x: 2, y: 2, z: 1, core: 2. Of those that a mesh axis runs over, the one named last changes fastest.
Arguments:
- x: bfloat16 [1792, 5120], P(('dp', 'tp'))
- w_gate: bfloat16 [5120, 12288], P(None, 'tp')
- w_up: bfloat16 [5120, 12288], P(None, 'tp')
- w_down: bfloat16 [12288, 5120], P('tp')
Outputs:
- output: bfloat16 [1792, 5120], P(('dp', 'tp'))
All inputs are finite; a program needn't handle non-finite values.
Results may differ from the reference program's by a relative error of at most 0.016.
Values are sent between devices in bfloat16 or wider.
A program may use at most 2 GiB of HBM per device.

```python
import jax
import jax.numpy as jnp

ROWS = 1792
D = 5120
FF = 12288


def setup_inputs(seed: int = 0, part: int = 0) -> dict:
    kx, kg, ku, kd = jax.random.split(jax.random.key(seed), 4)
    drawn = {
        "x": jax.random.normal(jax.random.fold_in(kx, part), (ROWS, D), jnp.float32),
        "w_gate": jax.random.normal(kg, (D, FF), jnp.float32) * D**-0.5,
        "w_up": jax.random.normal(ku, (D, FF), jnp.float32) * D**-0.5,
        "w_down": jax.random.normal(kd, (FF, D), jnp.float32) * FF**-0.5,
    }
    return {k: v.astype(jnp.bfloat16) for k, v in drawn.items()}


def reference(x, w_gate, w_up, w_down):
    gate = jnp.dot(x, w_gate, preferred_element_type=jnp.float32)
    up = jnp.dot(x, w_up, preferred_element_type=jnp.float32)
    hidden = (jax.nn.silu(gate) * up).astype(jnp.bfloat16)
    return jnp.dot(hidden, w_down, preferred_element_type=jnp.float32).astype(jnp.bfloat16)
```

```python
import functools

import jax
import jax.numpy as jnp
from jax import lax
from jax.experimental import pallas as pl
from jax.experimental.pallas import tpu as pltpu
from jax.sharding import PartitionSpec as P

MESH = pl.DeviceIdType.MESH
ROWS, D, F = 224, 5120, 1536
HALF = ROWS // 2
TG, TD = 256, 512
NG, ND = F // TG, D // TD
PIECE = 16
NP = HALF // PIECE
RING = 4
BF = jnp.bfloat16
F32 = jnp.float32


def events_done(slot):
    at = (3, 4, 5, 6, 7, 7, 7, 9, 10, 11, 12, 13, 14, 15, 16, 17, 18, 19, 20, 21, 22)
    n = 0
    for a in at:
        n = n + jnp.where(slot >= a, 1, 0)
    return n


def kernel(
    x, wg, wu, wd,
    y, xo, xf, s2, sib0,
    wgv, wuv, wdv, lhs, hid, ring, obuf, sib, diag,
    w_sem, wd_sem, lhs_sem, sx_sem, sy_sem, fwd_sem, d2d_sem, xo_sem, xf_sem,
    f_send, sib_recv, o1_send, o2_send, o3_send, s2_recv, diag_recv, o3_recv, y_sem, tail_sem,
    credit, nbr_credit,
):
    me = lax.axis_index("tp")
    xn, yn, core = me ^ 4, me ^ 2, me ^ 1
    A, B = pl.ds(0, HALF), pl.ds(HALF, HALF)

    def remote(src, dst, send, recv, to):
        return pltpu.make_async_remote_copy(
            src_ref=src, dst_ref=dst, send_sem=send, recv_sem=recv,
            device_id={"tp": to}, device_id_type=MESH,
        )

    def load_lhs(src, q):
        return pltpu.make_async_copy(src, lhs.at[lax.rem(q, 2)], lhs_sem.at[lax.rem(q, 2)])

    def load_w(src, dst, t, k):
        return pltpu.make_async_copy(src.at[:, pl.ds(t * TG, TG)], dst.at[t], w_sem.at[k, t])

    def load_wd(j):
        return pltpu.make_async_copy(wd.at[:, pl.ds(j * TD, TD)], wdv.at[j], wd_sem.at[j])

    pltpu.make_async_copy(x, lhs.at[0], lhs_sem.at[0]).start()
    for t in range(NG):
        load_w(wg, wgv, t, 0).start()
        load_w(wu, wuv, t, 1).start()

    barrier = pltpu.get_barrier_semaphore()
    for other in (xn, yn, core):
        pl.semaphore_signal(barrier, inc=1, device_id={"tp": other}, device_id_type=MESH)
    pl.semaphore_wait(barrier, 3)

    def piece(h, k):
        return pl.ds(pl.multiple_of(h * HALF + k * PIECE, PIECE), PIECE)

    def own_piece(g, h, k):
        r = piece(h, k)
        over_x = (h == 0) == (g == 0)
        return remote(x.at[r], xo.at[g, r], (sx_sem if over_x else sy_sem).at[0], xo_sem.at[g, h, k],
                      xn if over_x else yn)

    @pl.loop(0, NP)
    def _(k):
        own_piece(0, 0, k).start()
        own_piece(0, 1, k).start()

    remote(x, xf.at[0], d2d_sem.at[0], xf_sem.at[0], core).start()
    for j in range(ND):
        load_wd(j).start()

    def handle(e):
        g, k = e // NP, lax.rem(e, NP)
        for h in (0, 1):
            r = piece(h, k)
            rows = xo.at[g, r]
            remote(rows, rows, sx_sem.at[0], xo_sem.at[g, h, k], xn).wait_recv()
            remote(rows, xf.at[g + 1, r], d2d_sem.at[g + 1], xf_sem.at[g + 1], core).start()

            @pl.when(g == 0)
            def _():
                remote(rows, xo.at[1, r], fwd_sem.at[h], xo_sem.at[1, h, k], yn if h == 0 else xn).start()

        @pl.when(e == NP - 1)
        def _():
            @pl.loop(0, NP)
            def _(k):
                own_piece(2, 0, k).start()
                own_piece(2, 1, k).start()

    def run_events(slot):
        lo = events_done(slot - 1)
        hi = events_done(slot)

        @pl.loop(lo, hi)
        def _(e):
            handle(e)

    def load_partner(g, q):
        remote(xf.at[g], xf.at[g], d2d_sem.at[g], xf_sem.at[g], core).wait_recv()
        load_lhs(xf.at[g], q).start()

    def gate_up(q):
        @pl.when((q >= 2) & (lax.rem(q, 2) == 0))
        def _():
            load_lhs(xo.at[q // 2 - 1], q + 1).start()

        load_lhs(x, q).wait()
        rows = lhs.at[lax.rem(q, 2)]
        dst = hid.at[jnp.minimum(q, 1)]

        @pl.loop(0, NG)
        def _(t):
            @pl.when(q == 0)
            def _():
                load_w(wg, wgv, t, 0).wait()
                load_w(wu, wuv, t, 1).wait()

                @pl.when(t == NG - 2)
                def _():
                    load_partner(0, 1)

            gate = jnp.dot(rows[...], wgv[t], preferred_element_type=F32)
            up = jnp.dot(rows[...], wuv[t], preferred_element_type=F32)
            dst[:, pl.ds(pl.multiple_of(t * TG, TG), TG)] = (jax.nn.silu(gate) * up).astype(BF)

            @pl.when(lax.rem(t, 2) == 1)
            def _():
                run_events(4 * q + t // 2)

    def down(h, j):
        return jnp.dot(hid[h], wdv[j], preferred_element_type=F32)

    def f_copy(slot, j, g):
        dst = sib0.at[j] if g == 0 else sib.at[j]
        return remote(ring.at[slot], dst, f_send.at[slot], sib_recv.at[0 if g == 0 else 1], core)

    def f_down(q):
        @pl.when(q >= 4)
        def _():
            pl.semaphore_wait(credit, 1)

        base = ND * (q // 2)

        @pl.loop(0, ND)
        def _(j):
            slot = lax.rem(base + j, RING)

            @pl.when(q == 1)
            def _():
                load_wd(j).wait()

            @pl.when(base + j >= RING)
            def _():
                f_copy(slot, j, 1).wait_send()

            ring[slot] = down(1, j).astype(BF)

            @pl.when(q == 1)
            def _():
                f_copy(slot, j, 0).start()

            @pl.when(q > 1)
            def _():
                f_copy(slot, j, 1).start()

    def wait_sib():
        remote(sib, sib, f_send.at[0], sib_recv.at[1], core).wait_recv()

    def o_copy(src, dst, send, recv, j, h, to):
        r = A if h == 0 else B
        return remote(src.at[j, r], dst.at[j, r], send, recv, to)

    def o1_copy(j, h):
        return o_copy(obuf.at[0], s2, o1_send.at[h], s2_recv.at[h], j, h, xn if h == 0 else yn)

    def o2_copy(j, h):
        return o_copy(obuf.at[1], diag, o2_send.at[h, j], diag_recv.at[h, j], j, h, xn if h == 0 else yn)

    def o3_copy(j, h):
        return o_copy(obuf.at[1], obuf.at[0], o3_send.at[h], o3_recv.at[h, j], j, h, yn if h == 0 else xn)

    def half_wait(buf, send, recv, h, which):
        r = A if h == 0 else B
        c = remote(buf.at[:, r], buf.at[:, r], send, recv, xn)
        c.wait_send() if which == "send" else c.wait_recv()

    def o_down(q):
        wait_sib()

        @pl.loop(0, ND)
        def _(j):
            obuf[jnp.where(q == 3, 0, 1), j] = (down(1, j) + sib[j].astype(F32)).astype(BF)
            for h in (0, 1):
                @pl.when(q == 3)
                def _():
                    o1_copy(j, h).start()

                @pl.when(q == 5)
                def _():
                    o2_copy(j, h).start()

        pl.semaphore_signal(credit, inc=1, device_id={"tp": core}, device_id_type=MESH)

    def o_last():
        for h in (0, 1):
            half_wait(obuf.at[0], o1_send.at[h], s2_recv.at[h], h, "send")
        for other in (xn, yn):
            pl.semaphore_signal(nbr_credit, inc=1, device_id={"tp": other}, device_id_type=MESH)
        wait_sib()
        pl.semaphore_wait(nbr_credit, 2)

        @pl.loop(0, ND)
        def _(j):
            for h in (0, 1):
                o2_copy(j, h).wait_recv()
                o2_copy(j, h).wait_send()
            acc = down(1, j) + sib[j].astype(F32) + diag[j].astype(F32)
            obuf[1, j] = acc.astype(BF)
            for h in (0, 1):
                o3_copy(j, h).start()

    @pl.loop(0, 8)
    def _(q):
        gate_up(q)

        @pl.when((q == 1) | ((q >= 2) & (lax.rem(q, 2) == 0)))
        def _():
            f_down(q)

        @pl.when((q == 3) | (q == 5))
        def _():
            o_down(q)

        run_events(4 * q + 3)

        @pl.when((q == 1) | (q == 3) | (q == 5))
        def _():
            load_partner((q + 1) // 2, q + 1)

    o_last()

    load_sib0 = pltpu.make_async_copy(sib0, sib, tail_sem.at[0])
    load_s2 = pltpu.make_async_copy(s2, diag, tail_sem.at[1])
    remote(sib0, sib0, f_send.at[0], sib_recv.at[0], core).wait_recv()
    load_sib0.start()
    for h in (0, 1):
        half_wait(s2, o1_send.at[h], s2_recv.at[h], h, "recv")
    load_s2.start()
    for s in range(RING):
        f_copy(s, 0, 1).wait_send()
    load_sib0.wait()
    load_s2.wait()

    def y_copy(j):
        slot = lax.rem(j, RING)
        return pltpu.make_async_copy(
            ring.at[slot], y.at[:, pl.ds(pl.multiple_of(j * TD, TD), TD)], y_sem.at[slot]
        )

    @pl.loop(0, ND)
    def _(j):
        @pl.when(j >= RING)
        def _():
            y_copy(j).wait()

        acc = down(0, j) + sib[j].astype(F32) + diag[j].astype(F32)
        for h in (0, 1):
            o3_copy(j, h).wait_recv()
        ring[lax.rem(j, RING)] = (acc + obuf[0, j].astype(F32)).astype(BF)
        y_copy(j).start()

    for j in range(ND - RING, ND):
        y_copy(j).wait()

    remote(x, x, sx_sem.at[0], xf_sem.at[0], xn).wait_send()
    remote(x, x, sy_sem.at[0], xf_sem.at[0], yn).wait_send()
    for h in (0, 1):
        remote(x.at[A], x.at[A], fwd_sem.at[h], xf_sem.at[0], yn).wait_send()
        half_wait(obuf.at[1], o3_send.at[h], s2_recv.at[h], h, "send")
    for g in range(4):
        remote(x, x, d2d_sem.at[g], xf_sem.at[0], core).wait_send()


def solution(mesh):
    def step(x, w_gate, w_up, w_down):
        hbm = pl.BlockSpec(memory_space=pltpu.HBM)
        shape = lambda *s: jax.ShapeDtypeStruct(s, BF)
        dma, reg = pltpu.SemaphoreType.DMA, pltpu.SemaphoreType.REGULAR
        y, *_ = pl.pallas_call(
            kernel,
            out_shape=[
                shape(ROWS, D), shape(3, ROWS, D), shape(4, ROWS, D), shape(ND, ROWS, TD), shape(ND, ROWS, TD),
            ],
            in_specs=[hbm] * 4,
            out_specs=[hbm] * 5,
            scratch_shapes=[
                pltpu.VMEM((NG, D, TG), BF), pltpu.VMEM((NG, D, TG), BF), pltpu.VMEM((ND, F, TD), BF),
                pltpu.VMEM((2, ROWS, D), BF), pltpu.VMEM((2, ROWS, F), BF), pltpu.VMEM((RING, ROWS, TD), BF),
                pltpu.VMEM((2, ND, ROWS, TD), BF), pltpu.VMEM((ND, ROWS, TD), BF), pltpu.VMEM((ND, ROWS, TD), BF),
                dma((2, NG)), dma((ND,)), dma((2,)), dma((1,)), dma((1,)), dma((2,)), dma((4,)),
                dma((3, 2, NP)), dma((4,)),
                dma((RING,)), dma((2,)), dma((2,)), dma((2, ND)), dma((2,)), dma((2,)), dma((2, ND)),
                dma((2, ND)), dma((RING,)), dma((2,)),
                reg, reg,
            ],
            compiler_params=pltpu.CompilerParams(
                collective_id=0, has_side_effects=True, vmem_limit_bytes=67043328,
            ),
            name="mlp_block",
        )(x, w_gate, w_up, w_down)
        return y

    return jax.shard_map(
        step,
        mesh=mesh,
        in_specs=(P(("dp", "tp"), None), P(None, "tp"), P(None, "tp"), P("tp", None)),
        out_specs=P(("dp", "tp"), None),
        check_vma=False,
    )
```
